32 devices in a mesh: row: 8 (over y, x, core), col: 4 (over z).
Axes of the slice: x: 2, y: 2, z: 4, core: 2. Of those that a mesh axis runs over, the one named last changes fastest.
Arguments:
- queries: bfloat16 [8, 128, 4096], P(None, 'row', 'col'), may hold values from -13 to 13, as said below
- key_cache: bfloat16 [8, 16384, 1024], P(None, ('row', 'col')), may hold values from -13 to 13
- value_cache: bfloat16 [8, 16384, 1024], P(None, ('row', 'col')), may hold values from -6 to 6
- key_table: bfloat16 [1024, 1024], replicated, may hold values from -24 to 24
- value_table: bfloat16 [1024, 1024], replicated, may hold values from -6 to 6
- lengths: int32 [8], replicated, may hold values from 2048 to 16384
- token_ids: int32 [8, 128], P(None, 'row'), may hold values from 0 to 1023
Outputs:
- attended: bfloat16 [8, 128, 4096], P(None, 'row', 'col')
The draws below stay inside these ranges and needn't reach their ends.
Inputs may be any that keep to these rules, and one draw needn't show every extreme that they name: `queries`: entries of the query array lie in the stated range.
All inputs are finite; a program needn't handle non-finite values.
Results may differ from the reference program's by a relative error of at most 0.006.
Values may be sent and summed in bfloat16 or wider, within the bound.
A program may use at most 192 MiB of HBM per device.

```python
import jax
import jax.numpy as jnp
from jax import lax

USERS = 8
BEAMS = 128
L_DEV = 512
HQ = 32
KH = 8
HD = 128
VOCAB = 1024
CONTEXT = 16384


def anchor_parts(key):
    signs = jnp.where(jax.random.bernoulli(jax.random.fold_in(key, 4242), 0.5, (USERS, KH, HD)), 1.7, -1.7)
    places = jax.random.randint(jax.random.fold_in(key, 4243), (USERS,), 0, CONTEXT // 8 - 1)
    strength = jax.random.uniform(jax.random.fold_in(key, 4244), (USERS,), jnp.float32, 1.5, 4.0)
    return (signs.astype(jnp.float32), places, strength)


def draw_key_cache(key, part):
    base = jnp.clip(jax.random.normal(jax.random.fold_in(key, 11), (USERS, CONTEXT, KH * HD), jnp.float32), -6.0, 6.0)
    anchors, places, strength = anchor_parts(key)
    flat = anchors.reshape(USERS, 1, KH * HD)
    spots = jnp.arange(CONTEXT, dtype=jnp.int32)[None, :, None]
    base = jnp.where(spots == places[:, None, None], 4.0 * flat, base)
    base = jnp.where(spots == places[:, None, None] + 1, 3.96 * flat, base)
    return jnp.clip(base, -13.0, 13.0).astype(jnp.bfloat16)


def draw_queries(key, part):
    base = jnp.clip(jax.random.normal(jax.random.fold_in(key, 21), (USERS, BEAMS, HQ * HD), jnp.float32), -6.0, 6.0)
    anchors, places, strength = anchor_parts(key)
    factor = strength * (81.0 / (11.56 * HD ** 0.5))
    spread = jnp.repeat(anchors, HQ // KH, axis=1).reshape(USERS, 1, HQ * HD) * factor[:, None, None]
    beam_at = jnp.arange(BEAMS, dtype=jnp.int32)[None, :, None]
    base = jnp.where(beam_at == 0, spread, base)
    return jnp.clip(base, -13.0, 13.0).astype(jnp.bfloat16)


def set_ends(entries, rng, least, high):
    extent = entries.shape
    index_at = [jax.random.randint(jax.random.fold_in(rng, axis), (), 0, extent[axis]) for axis in range(len(extent))]
    entries = entries.at[tuple(index_at)].set(least)
    longest = extent.index(max(extent))
    index_at[longest] = (index_at[longest] + 1) % extent[longest]
    return entries.at[tuple(index_at)].set(high)


def levels(key, shape, pieces, least, top_value):
    def one(dim, parts):
        draws = jax.random.uniform(jax.random.fold_in(jax.random.fold_in(key, 6), dim), (parts,), jnp.float32, least / len(pieces), top_value / len(pieces))
        return jnp.repeat(jnp.exp(draws), shape[dim] // parts).reshape((-1,) + (1,) * (len(shape) - dim - 1))

    level = one(*pieces[0])
    for cut in pieces[1:]:
        level = level * one(*cut)
    return level


def noise(own_key, dims, width, reach, shards=(), held_as=jnp.bfloat16):
    level = levels(own_key, dims, shards, -0.22, 0.18) if shards else 1.0
    array = jax.random.normal(own_key, dims, jnp.float32) * width * level
    return jnp.minimum(jnp.maximum(array, -reach), reach).astype(held_as)


def setup_inputs(seed: int = 0) -> dict:
    streams_of = jax.random.split(jax.random.key(seed), 8)
    queries = draw_queries(jax.random.fold_in(streams_of[7], 71), 0)
    key_cache = draw_key_cache(jax.random.fold_in(streams_of[7], 71), 0)
    value_cache = noise(streams_of[2], (USERS, CONTEXT, KH * HD), 1.0, 6.0, ((1, 32),))
    key_table = noise(streams_of[3], (VOCAB, KH * HD), 4.0, 24.0)
    value_table = noise(streams_of[4], (VOCAB, KH * HD), 1.0, 6.0)
    lengths = set_ends(jax.random.randint(streams_of[5], (USERS,), CONTEXT // 8, CONTEXT + 1), jax.random.fold_in(streams_of[5], 1), CONTEXT // 8, CONTEXT).astype(jnp.int32)
    token_ids = set_ends(jax.random.randint(streams_of[6], (USERS, BEAMS), 0, VOCAB), jax.random.fold_in(streams_of[6], 1), 0, VOCAB - 1).astype(jnp.int32)
    return dict(queries=queries, key_cache=key_cache, value_cache=value_cache, key_table=key_table, value_table=value_table, lengths=lengths, token_ids=token_ids)


def reference(queries, key_cache, value_cache, key_table, value_table, lengths, token_ids):
    group = HQ // KH
    scale = HD ** -0.5
    blocks = CONTEXT // L_DEV
    q_all = queries.astype(jnp.float32).reshape(USERS, BEAMS, KH, group, HD)
    own_keys = key_table[token_ids].astype(jnp.float32).reshape(USERS, BEAMS, KH, 1, HD)
    own_values = value_table[token_ids].astype(jnp.float32).reshape(USERS, BEAMS, KH, 1, HD)
    own_scores = jnp.sum(q_all * own_keys, axis=-1) * scale
    starts = jnp.arange(blocks, dtype=jnp.int32) * L_DEV

    def per_user(items):
        q_user, k_user, v_user, limit, self_score, self_value = items
        k_blocks = k_user.reshape(blocks, L_DEV, KH, HD)
        v_blocks = v_user.reshape(blocks, L_DEV, KH, HD)

        def scores(k_blk, start):
            s = jnp.einsum('wkgd,lkd->wkgl', q_user, k_blk.astype(jnp.float32)) * scale
            live = (start + jnp.arange(L_DEV, dtype=jnp.int32)) < limit
            return jnp.where(live, s, -1e30), live

        def pass_max(peak, items):
            k_blk, start = items
            s, live = scores(k_blk, start)
            return jnp.maximum(peak, jnp.max(s, axis=-1)), None

        peak, _ = lax.scan(pass_max, self_score, (k_blocks, starts))
        first = jnp.exp(self_score - peak)

        def pass_sum(carry, items):
            total, numer = carry
            k_blk, v_blk, start = items
            s, live = scores(k_blk, start)
            weight = jnp.where(live, jnp.exp(s - peak[..., None]), 0.0)
            total = total + jnp.sum(weight, axis=-1)
            rounded = weight.astype(jnp.bfloat16).astype(jnp.float32)
            numer = numer + jnp.einsum('wkgl,lkd->wkgd', rounded, v_blk.astype(jnp.float32))
            return (total, numer), None

        init = (first, first[..., None] * self_value)
        (total, numer), _ = lax.scan(pass_sum, init, (k_blocks, v_blocks, starts))
        return (numer / total[..., None]).reshape(BEAMS, HQ * HD).astype(jnp.bfloat16)

    return lax.map(per_user, (q_all, key_cache, value_cache, lengths, own_scores, own_values))
```

```python
import math

import jax
import jax.numpy as jnp
from jax import lax
from jax.experimental import pallas as pl
from jax.experimental.pallas import tpu as pltpu
from jax.sharding import PartitionSpec as P

HQ = 32
KH = 8
HD = 128
GROUP = HQ // KH
CORES = 2
LOG2E = math.log2(math.e)
FACTOR = HD ** (-0.5) * LOG2E
MESH = pl.DeviceIdType.MESH
LEAD = 3
TAIL = 3


class Plan:
    def __init__(self, rows, cols):
        self.rows, self.cols = rows, cols
        self.planes = rows // CORES
        self.outer = 2 if self.planes % 2 == 0 else 1
        self.inner = self.planes // self.outer
        self.half = cols // 2
        names = []
        for s in range(1, cols):
            names += [("z", s), ("zr", s), ("zs", s)]
        for b in range(1, self.inner):
            names += [("bx", b), ("cd", b), ("x", b), ("xs", b)]
        for a in range(1, self.outer):
            names += [("by", a), ("ce", a), ("y", a), ("ys", a)]
            for b in range(1, self.inner):
                names += [(n, a, b) for n in ("ca", "cb", "dd", "ra", "ras", "rb", "rbs")]
        names += [("bd",), ("f",), ("fs",), ("fo",)]
        self.index = {name: at for at, name in enumerate(names)}


def step_kernel(
    plan, live_ref, q_in, k_hbm, v_hbm, out_ref, st_out,
    q_all, part, from_pair, st, st_pair, sc, ra, ras, rb, rbs, xr, xrs, yr, yrs, zr, zrs, fin,
    kbuf, vbuf, send, recv, local,
):
    users = q_in.shape[0]
    outer, inner, cols, half = plan.outer, plan.inner, plan.cols, plan.half
    planes = plan.planes
    kv = KH // cols
    lines = q_in.shape[1] // kv
    lanes = CORES * lines
    positions = k_hbm.shape[1]
    row, col = lax.axis_index("row"), lax.axis_index("col")
    k = lax.rem(row, CORES)
    pair = 1 - k
    me = row // CORES
    b_at, a_at = lax.rem(me, inner), me // inner

    def spot(a=0, b=0):
        return lax.rem(a_at + a + outer, outer) * inner + lax.rem(b_at + b + inner, inner)

    def at_spot(a=0, b=0):
        return {"row": spot(a, b) * CORES + k}

    def at_col(s):
        return {"col": lax.rem(col + s, cols)}

    at_pair = {"row": me * CORES + pair}
    in_x = range(1, inner)
    in_y = range(1, outer)
    in_xy = [(a, b) for a in in_y for b in in_x]
    in_z = range(1, cols)

    peers = [at_pair] + [at_col(s) for s in in_z] + [at_spot(0, b) for b in in_x] + [at_spot(a, 0) for a in in_y]

    def copy(v, name, src, dst, to):
        at = plan.index[name]
        return pltpu.make_async_remote_copy(
            src_ref=src, dst_ref=dst, send_sem=send.at[v, at], recv_sem=recv.at[v, at],
            device_id=to, device_id_type=MESH,
        )

    low, high = pl.ds(0, half), pl.ds(half, cols - half)

    def make(v, name):
        kind, *at = name
        if kind == "z":
            return copy(v, name, q_in.at[v], q_all.at[v, me, k, col], at_col(at[0]))
        if kind in ("bx", "by", "bd"):
            to = at_pair if kind == "bd" else at_spot(0, at[0]) if kind == "bx" else at_spot(at[0], 0)
            own = q_all.at[v, me, k]
            return copy(v, name, own, own, to)
        if kind == "cd":
            ref = q_all.at[v, spot(0, -at[0]), k]
            return copy(v, name, ref, ref, at_pair)
        if kind == "ce":
            ref = q_all.at[v, spot(-at[0], 0), k]
            return copy(v, name, ref, ref, at_pair)
        if kind == "ca":
            ref = q_all.at[v, spot(0, -at[1]), k, low]
            return copy(v, name, ref, ref, at_spot(at[0], 0))
        if kind == "cb":
            ref = q_all.at[v, spot(-at[0], 0), k, high]
            return copy(v, name, ref, ref, at_spot(0, at[1]))
        if kind == "dd":
            ref = q_all.at[v, spot(-at[0], -at[1]), k]
            return copy(v, name, ref, ref, at_pair)
        if kind == "f":
            return copy(v, name, part.at[v, pair], from_pair.at[v], at_pair)
        if kind == "fs":
            return copy(v, name, st.at[v], st_pair.at[v], at_pair)
        if kind == "ra":
            return copy(v, name, part.at[v, k, spot(*at), low], ra.at[v, at[0] - 1, at[1] - 1], at_spot(at[0], 0))
        if kind == "ras":
            return copy(v, name, sc.at[v, spot(*at), low], ras.at[v, at[0] - 1, at[1] - 1], at_spot(at[0], 0))
        if kind == "rb":
            return copy(v, name, part.at[v, k, spot(*at), high], rb.at[v, at[0] - 1, at[1] - 1], at_spot(0, at[1]))
        if kind == "rbs":
            return copy(v, name, sc.at[v, spot(*at), high], rbs.at[v, at[0] - 1, at[1] - 1], at_spot(0, at[1]))
        if kind == "x":
            return copy(v, name, part.at[v, k, spot(0, at[0])], xr.at[v, at[0] - 1], at_spot(0, at[0]))
        if kind == "xs":
            return copy(v, name, sc.at[v, spot(0, at[0])], xrs.at[v, at[0] - 1], at_spot(0, at[0]))
        if kind == "y":
            return copy(v, name, part.at[v, k, spot(at[0], 0)], yr.at[v, at[0] - 1], at_spot(at[0], 0))
        if kind == "ys":
            return copy(v, name, sc.at[v, spot(at[0], 0)], yrs.at[v, at[0] - 1], at_spot(at[0], 0))
        if kind == "zr":
            there = lax.rem(col + at[0], cols)
            return copy(v, name, part.at[v, k, me, there], zr.at[v, at[0] - 1], at_col(at[0]))
        if kind == "zs":
            there = lax.rem(col + at[0], cols)
            return copy(v, name, sc.at[v, me, there], zrs.at[v, at[0] - 1], at_col(at[0]))
        return copy(v, name, fin.at[v, k], fin.at[v, k], at_pair)

    def start(v, *names):
        for name in names:
            make(v, name).start()

    def arrived(v, *names):
        for name in names:
            make(v, name).wait_recv()

    def when(v, fn):
        @pl.when((v >= 0) & (v < users))
        def _():
            fn(v)

    def own_copy():
        return pltpu.make_async_copy(q_in, q_all.at[:, me, k, col], local.at[0])

    def fetch(v):
        slot = lax.rem(v, 2)
        return (
            pltpu.make_async_copy(k_hbm.at[v], kbuf.at[slot], local.at[1 + slot]),
            pltpu.make_async_copy(v_hbm.at[v], vbuf.at[slot], local.at[3 + slot]),
        )

    def start_fetch(v):
        for c in fetch(v):
            c.start()

    def columns(v):
        arrived(v, *[("z", s) for s in in_z])
        start(v, *[("bx", b) for b in in_x], *[("by", a) for a in in_y], ("bd",))

    def relay(v):
        for b in in_x:
            arrived(v, ("bx", b))
            start(v, *[("ca", a, b) for a in in_y], ("cd", b))
        for a in in_y:
            arrived(v, ("by", a))
            start(v, *[("cb", a, b) for b in in_x], ("ce", a))

    def diagonal(v):
        for a, b in in_xy:
            arrived(v, ("ca", a, b), ("cb", a, b))
            start(v, ("dd", a, b))

    def gathered(v):
        arrived(v, ("bd",), *[("cd", b) for b in in_x], *[("ce", a) for a in in_y])
        arrived(v, *[("dd", a, b) for a, b in in_xy])

    def heads(v, some):
        slot = lax.rem(v, 2)
        keep = lax.broadcasted_iota(jnp.int32, (positions, planes * lanes), 0) < live_ref[v]
        for j in some:
            c, i = divmod(j, kv)
            q = q_all[v, :, :, c, i * lines : (i + 1) * lines, :].reshape(planes * lanes, HD)
            keys = kbuf[slot, :, j * HD : (j + 1) * HD]
            s = lax.dot_general(keys, q, (((1,), (1,)), ((), ())), preferred_element_type=jnp.float32)
            s = jnp.where(keep, s, -1e30)
            m = jnp.max(s, axis=0, keepdims=True)
            p = jnp.exp2((s - m) * FACTOR)
            total = jnp.sum(p, axis=0, keepdims=True)
            m = m * FACTOR
            values = vbuf[slot, :, j * HD : (j + 1) * HD]
            o = lax.dot_general(
                values, p.astype(jnp.bfloat16), (((0,), (0,)), ((), ())), preferred_element_type=jnp.float32
            ).astype(jnp.bfloat16)
            for at in range(planes):
                span = slice(at * lanes, (at + 1) * lanes)
                st[v, at, c, i : i + 1, :] = m[:, span]
                st[v, at, c, kv + i : kv + i + 1, :] = total[:, span]
                for h in range(2):
                    part[v, h, at, c, i] = o[h * (HD // 2) : (h + 1) * (HD // 2), span]

    def fuse(numers, stats):
        peaks = [x[:kv] for x in stats]
        peak = peaks[0]
        for x in peaks[1:]:
            peak = jnp.maximum(peak, x)
        scales = [jnp.exp2(x - peak) for x in peaks]
        total = sum(x[kv:] * scale for x, scale in zip(stats, scales))
        sums = [
            sum(x[i].astype(jnp.float32) * scale[i : i + 1] for x, scale in zip(numers, scales))
            for i in range(kv)
        ]
        return sums, peak, total

    def fuse_into(v, at, c, numers, stats, first=None):
        own = part.at[v, k, at, c]
        own_st = sc.at[v, at, c]
        given = own_st if first is None else first
        sums, peak, total = fuse([own] + numers, [given[...]] + stats)
        for i in range(kv):
            own[i] = sums[i].astype(jnp.bfloat16)
        own_st[:kv] = peak
        own_st[kv:] = total

    def paired(v):
        arrived(v, ("f",), ("fs",))

        def one(at, _):
            for c in range(cols):
                fuse_into(v, at, c, [from_pair.at[v, at, c]], [st_pair[v, at, c]], st.at[v, at, c])
            return 0

        lax.fori_loop(0, planes, one, 0)
        for a, b in in_xy:
            start(v, ("ra", a, b), ("ras", a, b), ("rb", a, b), ("rbs", a, b))

    def crossed(v):
        for a, b in in_xy:
            arrived(v, ("ra", a, b), ("ras", a, b))
        for b in in_x:
            if in_y:
                for c in range(half):
                    fuse_into(
                        v, spot(0, b), c,
                        [ra.at[v, a - 1, b - 1, c] for a in in_y], [ras[v, a - 1, b - 1, c] for a in in_y],
                    )
            start(v, ("x", b), ("xs", b))
        for a, b in in_xy:
            arrived(v, ("rb", a, b), ("rbs", a, b))
        for a in in_y:
            if in_x:
                for c in range(cols - half):
                    fuse_into(
                        v, spot(a, 0), half + c,
                        [rb.at[v, a - 1, b - 1, c] for b in in_x], [rbs[v, a - 1, b - 1, c] for b in in_x],
                    )
            start(v, ("y", a), ("ys", a))

    def reduced(v):
        for b in in_x:
            arrived(v, ("x", b), ("xs", b))
        for a in in_y:
            arrived(v, ("y", a), ("ys", a))
        for c in range(cols):
            fuse_into(
                v, me, c,
                [xr.at[v, b - 1, c] for b in in_x] + [yr.at[v, a - 1, c] for a in in_y],
                [xrs[v, b - 1, c] for b in in_x] + [yrs[v, a - 1, c] for a in in_y],
            )
        for s in in_z:
            start(v, ("zr", s), ("zs", s))

    def finished(v):
        for s in in_z:
            arrived(v, ("zr", s), ("zs", s))
        sums, peak, total = fuse(
            [part.at[v, k, me, col]] + [zr.at[v, s - 1] for s in in_z],
            [sc[v, me, col]] + [zrs[v, s - 1] for s in in_z],
        )
        for i in range(kv):
            fin[v, k, i] = sums[i]
        st_out[v, :kv] = peak
        st_out[v, kv:] = total
        start(v, ("fo",))

    own_copy().start()
    start_fetch(0)
    barrier = pltpu.get_barrier_semaphore()
    for to in peers:
        pl.semaphore_signal(barrier, inc=1, device_id=to, device_id_type=MESH)
    pl.semaphore_wait(barrier, len(peers))

    def send_queries(v, _):
        start(v, *[("z", s) for s in in_z])
        return 0

    lax.fori_loop(0, users, send_queries, 0)
    own_copy().wait()

    def turn(t, _):
        u = t - LEAD
        when(u + 3, columns)

        @pl.when((u >= 0) & (u + 1 < users))
        def _():
            start_fetch(u + 1)

        def begin(v):
            gathered(v)
            for c in fetch(v):
                c.wait()
            heads(v, range(0, KH // 4))

        when(u, begin)
        when(u - 1, paired)
        when(u, lambda v: heads(v, range(KH // 4, KH // 2)))
        when(u + 2, relay)
        when(u - 2, reduced)
        when(u, lambda v: heads(v, range(KH // 2, 3 * KH // 4)))
        when(u - 1, crossed)

        def end(v):
            heads(v, range(3 * KH // 4, KH))
            start(v, ("f",), ("fs",))

        when(u, end)
        when(u + 1, diagonal)
        when(u - 3, finished)
        return 0

    lax.fori_loop(0, users + LEAD + TAIL, turn, 0)

    def close(v, _):
        arrived(v, ("fo",))
        out_ref[v] = fin[v]
        for name in plan.index:
            make(v, name).wait_send()
        return 0

    lax.fori_loop(0, users, close, 0)


def step(live, q_local, keys, values, rows, cols):
    users, piece, _ = q_local.shape
    plan = Plan(rows, cols)
    _, positions, width = keys.shape
    kv = KH // cols
    lanes = CORES * piece // kv
    outer, inner, planes, half = plan.outer, plan.inner, plan.planes, plan.half
    deep = HD // 2
    f32, bf16 = jnp.float32, jnp.bfloat16
    vmem = pl.BlockSpec(memory_space=pltpu.VMEM)
    hbm = pl.BlockSpec(memory_space=pl.ANY)
    block, stat = (kv, deep, lanes), (2 * kv, lanes)

    def numer(*lead):
        return pltpu.VMEM((users, *lead, *block), bf16)

    def stats(*lead):
        return pltpu.VMEM((users, *lead, *stat), f32)

    x, y = max(inner - 1, 1), max(outer - 1, 1)
    copies = len(plan.index)
    scores = users * KH * planes * lanes * positions
    return pl.pallas_call(
        lambda *refs: step_kernel(plan, *refs),
        out_shape=[
            jax.ShapeDtypeStruct((users, 2, *block), f32),
            jax.ShapeDtypeStruct((users, *stat), f32),
        ],
        in_specs=[pl.BlockSpec(memory_space=pltpu.SMEM), vmem, hbm, hbm],
        out_specs=[vmem, vmem],
        scratch_shapes=[
            pltpu.VMEM((users, planes, CORES, cols, piece, HD), bf16),
            numer(2, planes, cols),
            numer(planes, cols),
            stats(planes, cols),
            stats(planes, cols),
            stats(planes, cols),
            numer(y, x, half),
            stats(y, x, half),
            numer(y, x, cols - half),
            stats(y, x, cols - half),
            numer(x, cols),
            stats(x, cols),
            numer(y, cols),
            stats(y, cols),
            numer(cols - 1),
            stats(cols - 1),
            pltpu.VMEM((users, 2, *block), f32),
            pltpu.VMEM((2, positions, width), bf16),
            pltpu.VMEM((2, positions, width), bf16),
            pltpu.SemaphoreType.DMA((users, copies)),
            pltpu.SemaphoreType.DMA((users, copies)),
            pltpu.SemaphoreType.DMA((5,)),
        ],
        compiler_params=pltpu.CompilerParams(
            collective_id=0, has_side_effects=True, vmem_limit_bytes=60 * 1024 * 1024
        ),
        cost_estimate=pl.CostEstimate(
            flops=4 * scores * HD, bytes_accessed=4 * users * positions * width, transcendentals=scores
        ),
        name="step",
    )(live, q_local, keys, values)


def body(queries, key_cache, value_cache, key_table, value_table, lengths, token_ids):
    users, beam_part, width_part = queries.shape
    heads_part = width_part // HD
    kv_part = heads_part // GROUP
    rows, cols = lax.axis_size("row"), lax.axis_size("col")
    row_at, col_at = lax.axis_index("row"), lax.axis_index("col")
    positions = key_cache.shape[1]
    offset = (row_at * cols + col_at) * positions
    live = jnp.clip(lengths - offset, 0, positions)
    piece = heads_part * beam_part
    q_local = queries.reshape(users, beam_part, heads_part, HD).transpose(0, 2, 1, 3)
    q_local = q_local.reshape(users, piece, HD)

    own_keys, own_values = (
        jnp.einsum(
            "uwv,vc->uwc",
            (token_ids[..., None] == jnp.arange(table.shape[0], dtype=jnp.int32)).astype(jnp.bfloat16),
            lax.dynamic_slice_in_dim(table, col_at * kv_part * HD, kv_part * HD, 1),
            preferred_element_type=jnp.float32,
        )
        .reshape(users, beam_part, kv_part, HD)
        .transpose(0, 2, 1, 3)[:, :, None]
        for table in (key_table, value_table)
    )
    q_heads = q_local.astype(jnp.float32).reshape(users, kv_part, GROUP, beam_part, HD)
    own_score = jnp.sum(q_heads * own_keys, axis=-1) * FACTOR

    numer, stat = step(live, q_local, key_cache, value_cache, rows, cols)
    lines = GROUP * beam_part
    mine = lax.rem(row_at, CORES) * lines
    numer = lax.dynamic_slice_in_dim(numer, mine, lines, 4)
    numer = numer.transpose(0, 2, 4, 1, 3).reshape(users, kv_part, GROUP, beam_part, HD)
    stat = lax.dynamic_slice_in_dim(stat, mine, lines, 2).reshape(users, 2, kv_part, GROUP, beam_part)
    peak, total = stat[:, 0], stat[:, 1]
    top = jnp.maximum(peak, own_score)
    carried = jnp.exp2(peak - top)
    fresh = jnp.exp2(own_score - top)
    numer = numer * carried[..., None] + fresh[..., None] * own_values
    result = numer / (total * carried + fresh)[..., None]
    result = result.reshape(users, heads_part, beam_part, HD)
    return result.transpose(0, 2, 1, 3).reshape(users, beam_part, width_part).astype(jnp.bfloat16)


def solution(mesh):
    return jax.shard_map(
        body,
        mesh=mesh,
        in_specs=(
            P(None, "row", "col"),
            P(None, ("row", "col"), None),
            P(None, ("row", "col"), None),
            P(),
            P(),
            P(),
            P(None, "row"),
        ),
        out_specs=P(None, "row", "col"),
        check_vma=False,
    )
```

```python
import math

import jax
import jax.numpy as jnp
import numpy as np
from jax import lax
from jax.experimental import pallas as pl
from jax.experimental.pallas import tpu as pltpu
from jax.sharding import PartitionSpec as P

HQ = 32
KH = 8
HD = 128
GROUP = HQ // KH
CORES = 2
LOG2E = math.log2(math.e)
FACTOR = HD ** (-0.5) * LOG2E
MESH = pl.DeviceIdType.MESH
STEPS = (
    ("diagonal", 2, 0, 3),
    ("finished", -17, 1, 0),
    ("delivered", -39, 4, 1),
    ("relay", 4, 1, 1),
    ("reduced", -17, 8, 0),
    ("paired", -3, 2, 0),
    ("columns", 7, 1, 4),
    ("crossed", -13, 8, 0),
    ("attend", 1, 0, 0),
)
NEEDS = (
    ("columns", "relay"), ("relay", "diagonal"), ("diagonal", "attend"), ("attend", "paired"), ("paired", "crossed"),
    ("crossed", "reduced"), ("reduced", "finished"), ("finished", "delivered"),
)


def upto(chunks, base, early, late, u, lib):
    some = base + u + lib.minimum(lib.maximum(u, 0), early) + late * lib.maximum(u - (chunks - 1), 0)
    return lib.minimum(lib.maximum(some, 0), chunks)


def turns(chunks):
    first = -max(base for _, base, _, _ in STEPS)
    last, order = first, {}
    while last < chunks or any(upto(chunks, *rest, last - 1, np) < chunks for _, *rest in STEPS):
        for name, *rest in STEPS:
            for v in range(upto(chunks, *rest, last - 1, np), upto(chunks, *rest, last, np)):
                order[name, v] = len(order)
        last += 1
    for before, after in NEEDS:
        assert all(order[before, v] < order[after, v] for v in range(chunks)), (before, after)
    return first, last


class Plan:
    def __init__(self, rows, cols):
        self.rows, self.cols = rows, cols
        self.planes = rows // CORES
        self.outer = 2 if self.planes % 2 == 0 else 1
        self.inner = self.planes // self.outer
        self.half = cols // 2
        names = []
        for s in range(1, cols):
            names += [("z", s), ("zr", s), ("zs", s)]
        for b in range(1, self.inner):
            names += [("bx", b), ("cd", b), ("x", b), ("xs", b)]
        for a in range(1, self.outer):
            names += [("by", a), ("ce", a), ("y", a), ("ys", a)]
            for b in range(1, self.inner):
                names += [(n, a, b) for n in ("ca", "cb", "dd", "ra", "ras", "rb", "rbs")]
        names += [("bd",), ("f",), ("fs",), ("fo",)]
        self.index = {name: at for at, name in enumerate(names)}


def step_kernel(
    plan, len_ref, tok_ref, q_hbm, k_hbm, v_hbm, kt_hbm, vt_hbm, out_ref,
    q_in, ktab, vtab, own_e, own_w, turned, turned_st, fin_st,
    q_all, part, from_pair, st, st_pair, sc, ra, ras, rb, rbs, xr, xrs, yr, yrs, zr, zrs, fin,
    kbuf, vbuf, send, recv, local,
):
    chunks = q_in.shape[0]
    outer, inner, cols, half = plan.outer, plan.inner, plan.cols, plan.half
    planes = plan.planes
    kv = KH // cols
    beams = q_in.shape[2]
    lines = GROUP * beams
    lanes = CORES * lines
    positions = k_hbm.shape[1]
    users = k_hbm.shape[0]
    vocab = ktab.shape[0]
    row, col = lax.axis_index("row"), lax.axis_index("col")
    k = lax.rem(row, CORES)
    pair = 1 - k
    me = row // CORES
    b_at, a_at = lax.rem(me, inner), me // inner
    offset = (row * cols + col) * positions

    def spot(a=0, b=0):
        return lax.rem(a_at + a + outer, outer) * inner + lax.rem(b_at + b + inner, inner)

    def at_spot(a=0, b=0):
        return {"row": spot(a, b) * CORES + k}

    def at_col(s):
        return {"col": lax.rem(col + s, cols)}

    at_pair = {"row": me * CORES + pair}
    in_x = range(1, inner)
    in_y = range(1, outer)
    in_xy = [(a, b) for a in in_y for b in in_x]
    in_z = range(1, cols)

    peers = [at_pair] + [at_col(s) for s in in_z] + [at_spot(0, b) for b in in_x] + [at_spot(a, 0) for a in in_y]

    def copy(v, name, src, dst, to):
        at = plan.index[name]
        return pltpu.make_async_remote_copy(
            src_ref=src, dst_ref=dst, send_sem=send.at[v, at], recv_sem=recv.at[v, at],
            device_id=to, device_id_type=MESH,
        )

    low, high = pl.ds(0, half), pl.ds(half, cols - half)

    def make(v, name):
        kind, *at = name
        if kind == "z":
            return copy(v, name, q_in.at[v], q_all.at[v, me, k, col], at_col(at[0]))
        if kind in ("bx", "by", "bd"):
            to = at_pair if kind == "bd" else at_spot(0, at[0]) if kind == "bx" else at_spot(at[0], 0)
            own = q_all.at[v, me, k]
            return copy(v, name, own, own, to)
        if kind == "cd":
            ref = q_all.at[v, spot(0, -at[0]), k]
            return copy(v, name, ref, ref, at_pair)
        if kind == "ce":
            ref = q_all.at[v, spot(-at[0], 0), k]
            return copy(v, name, ref, ref, at_pair)
        if kind == "ca":
            ref = q_all.at[v, spot(0, -at[1]), k, low]
            return copy(v, name, ref, ref, at_spot(at[0], 0))
        if kind == "cb":
            ref = q_all.at[v, spot(-at[0], 0), k, high]
            return copy(v, name, ref, ref, at_spot(0, at[1]))
        if kind == "dd":
            ref = q_all.at[v, spot(-at[0], -at[1]), k]
            return copy(v, name, ref, ref, at_pair)
        if kind == "f":
            return copy(v, name, part.at[v, pair], from_pair.at[v], at_pair)
        if kind == "fs":
            return copy(v, name, st.at[v], st_pair.at[v], at_pair)
        if kind == "ra":
            return copy(v, name, part.at[v, k, spot(*at), low], ra.at[v, at[0] - 1, at[1] - 1], at_spot(at[0], 0))
        if kind == "ras":
            return copy(v, name, sc.at[v, spot(*at), low], ras.at[v, at[0] - 1, at[1] - 1], at_spot(at[0], 0))
        if kind == "rb":
            return copy(v, name, part.at[v, k, spot(*at), high], rb.at[v, at[0] - 1, at[1] - 1], at_spot(0, at[1]))
        if kind == "rbs":
            return copy(v, name, sc.at[v, spot(*at), high], rbs.at[v, at[0] - 1, at[1] - 1], at_spot(0, at[1]))
        if kind == "x":
            return copy(v, name, part.at[v, k, spot(0, at[0])], xr.at[v, at[0] - 1], at_spot(0, at[0]))
        if kind == "xs":
            return copy(v, name, sc.at[v, spot(0, at[0])], xrs.at[v, at[0] - 1], at_spot(0, at[0]))
        if kind == "y":
            return copy(v, name, part.at[v, k, spot(at[0], 0)], yr.at[v, at[0] - 1], at_spot(at[0], 0))
        if kind == "ys":
            return copy(v, name, sc.at[v, spot(at[0], 0)], yrs.at[v, at[0] - 1], at_spot(at[0], 0))
        if kind == "zr":
            there = lax.rem(col + at[0], cols)
            return copy(v, name, part.at[v, k, me, there], zr.at[v, at[0] - 1], at_col(at[0]))
        if kind == "zs":
            there = lax.rem(col + at[0], cols)
            return copy(v, name, sc.at[v, me, there], zrs.at[v, at[0] - 1], at_col(at[0]))
        return copy(v, name, fin.at[v, k], fin.at[v, k], at_pair)

    def start(v, *names):
        for name in names:
            make(v, name).start()

    def arrived(v, *names):
        for name in names:
            make(v, name).wait_recv()

    def own_copy():
        return pltpu.make_async_copy(q_in, q_all.at[:, me, k, col], local.at[0])

    spare = 1 + 4 * cols
    wide = pl.ds(pl.multiple_of(col * kv * HD, HD), kv * HD)
    taken = [
        pltpu.make_async_copy(
            q_hbm.at[u, :, pl.ds((i * GROUP + g) * HD, HD)],
            q_in.at[u * kv + i, g],
            local.at[spare + (u * kv + i) * GROUP + g],
        )
        for u in range(users)
        for i in range(kv)
        for g in range(GROUP)
    ]
    spare += len(taken)
    tables = [
        pltpu.make_async_copy(kt_hbm.at[:, wide], ktab, local.at[spare]),
        pltpu.make_async_copy(vt_hbm.at[:, wide], vtab, local.at[spare + 1]),
    ]

    def own_terms(u, _):
        pick = lax.broadcasted_iota(jnp.int32, (vocab, beams), 0) == tok_ref[pl.ds(u, 1), :]
        pick = jnp.where(pick, 1.0, 0.0).astype(jnp.bfloat16)
        found, own_w[u] = (
            lax.dot_general(pick, tab[...], (((0,), (0,)), ((), ())), preferred_element_type=jnp.float32)
            for tab in (ktab, vtab)
        )
        for i in range(kv):
            keys = found[:, i * HD : (i + 1) * HD]
            for g in range(GROUP):
                q = q_in[u * kv + i, g].astype(jnp.float32)
                own_e[u * kv + i, g * beams : (g + 1) * beams] = jnp.sum(q * keys, axis=1, keepdims=True) * FACTOR
        return 0

    def fetch(v):
        slot = lax.rem(v, 2)
        found = []
        for c in range(cols):
            at = pl.ds(pl.multiple_of((c * kv + lax.rem(v, kv)) * HD, HD), HD)
            for n, (src, dst) in enumerate([(k_hbm, kbuf), (v_hbm, vbuf)]):
                found.append(
                    pltpu.make_async_copy(src.at[v // kv, :, at], dst.at[slot, c], local.at[1 + (c * 2 + n) * 2 + slot])
                )
        return found

    def start_fetch(v):
        for c in fetch(v):
            c.start()

    def columns(v):
        arrived(v, *[("z", s) for s in in_z])
        start(v, *[("bx", b) for b in in_x], *[("by", a) for a in in_y], ("bd",))

    def relay(v):
        for b in in_x:
            arrived(v, ("bx", b))
            start(v, *[("ca", a, b) for a in in_y], ("cd", b))
        for a in in_y:
            arrived(v, ("by", a))
            start(v, *[("cb", a, b) for b in in_x], ("ce", a))

    def diagonal(v):
        for a, b in in_xy:
            arrived(v, ("ca", a, b), ("cb", a, b))
            start(v, ("dd", a, b))

    def gathered(v):
        arrived(v, ("bd",), *[("cd", b) for b in in_x], *[("ce", a) for a in in_y])
        arrived(v, *[("dd", a, b) for a, b in in_xy])

    def heads(v, some):
        slot = lax.rem(v, 2)
        keep = lax.broadcasted_iota(jnp.int32, (positions, planes * lanes), 0) < len_ref[v // kv] - offset
        for c in some:
            q = q_all[v, :, :, c].reshape(planes * lanes, HD)
            s = lax.dot_general(kbuf[slot, c], q, (((1,), (1,)), ((), ())), preferred_element_type=jnp.float32)
            s = jnp.where(keep, s, -1e30)
            m = jnp.max(s, axis=0, keepdims=True)
            p = jnp.exp2((s - m) * FACTOR)
            total = jnp.sum(p, axis=0, keepdims=True)
            m = m * FACTOR
            o = lax.dot_general(
                vbuf[slot, c], p.astype(jnp.bfloat16), (((0,), (0,)), ((), ())), preferred_element_type=jnp.float32
            ).astype(jnp.bfloat16)
            for at in range(planes):
                span = slice(at * lanes, (at + 1) * lanes)
                st[v, at, c, :1, :] = m[:, span]
                st[v, at, c, 1:, :] = total[:, span]
                for h in range(2):
                    part[v, h, at, c] = o[h * (HD // 2) : (h + 1) * (HD // 2), span]

    def fuse(numers, stats):
        peaks = [x[..., :1, :] for x in stats]
        peak = peaks[0]
        for x in peaks[1:]:
            peak = jnp.maximum(peak, x)
        scales = [jnp.exp2(x - peak) for x in peaks]
        total = sum(x[..., 1:, :] * scale for x, scale in zip(stats, scales))
        numer = sum(x.astype(jnp.float32) * scale for x, scale in zip(numers, scales))
        return numer, peak, total

    def put(v, at, span, numer, peak, total):
        part[v, k, at, span] = numer.astype(jnp.bfloat16)
        sc[v, at, span, :1, :] = peak
        sc[v, at, span, 1:, :] = total

    def fuse_into(v, at, span, numers, stats):
        put(v, at, span, *fuse([part[v, k, at, span]] + numers, [sc[v, at, span]] + stats))

    def paired(v):
        arrived(v, ("f",), ("fs",))
        for at in range(planes):
            put(
                v, at, pl.ds(0, cols),
                *fuse([part[v, k, at], from_pair[v, at]], [st[v, at], st_pair[v, at]]),
            )
        for a, b in in_xy:
            start(v, ("ra", a, b), ("ras", a, b), ("rb", a, b), ("rbs", a, b))

    def crossed(v):
        for a, b in in_xy:
            arrived(v, ("ra", a, b), ("ras", a, b), ("rb", a, b), ("rbs", a, b))
        if in_xy:
            for b in in_x:
                fuse_into(
                    v, spot(0, b), low,
                    [ra[v, a - 1, b - 1] for a in in_y], [ras[v, a - 1, b - 1] for a in in_y],
                )
            for a in in_y:
                fuse_into(
                    v, spot(a, 0), high,
                    [rb[v, a - 1, b - 1] for b in in_x], [rbs[v, a - 1, b - 1] for b in in_x],
                )
        for b in in_x:
            start(v, ("x", b), ("xs", b))
        for a in in_y:
            start(v, ("y", a), ("ys", a))

    def reduced(v):
        for b in in_x:
            arrived(v, ("x", b), ("xs", b))
        for a in in_y:
            arrived(v, ("y", a), ("ys", a))
        fuse_into(
            v, me, pl.ds(0, cols),
            [xr[v, b - 1] for b in in_x] + [yr[v, a - 1] for a in in_y],
            [xrs[v, b - 1] for b in in_x] + [yrs[v, a - 1] for a in in_y],
        )
        for s in in_z:
            start(v, ("zr", s), ("zs", s))

    def finished(v):
        for s in in_z:
            arrived(v, ("zr", s), ("zs", s))
        numer, peak, total = fuse(
            [part[v, k, me, col]] + [zr[v, s - 1] for s in in_z],
            [sc[v, me, col]] + [zrs[v, s - 1] for s in in_z],
        )
        fin[v, k] = numer
        fin_st[v, :1] = peak
        fin_st[v, 1:2] = total
        start(v, ("fo",))

    def delivered(v):
        arrived(v, ("fo",))
        turned[...] = fin[v].reshape(HD, lanes).T
        turned_st[...] = fin_st[v].T
        mine = pl.ds(pl.multiple_of(k * lines, lines), lines)
        numer = turned[mine, :]
        peak, total = turned_st[mine, 0:1], turned_st[mine, 1:2]
        own = own_e[v]
        top = jnp.maximum(peak, own)
        carried, fresh = jnp.exp2(peak - top), jnp.exp2(own - top)
        u, i = v // kv, lax.rem(v, kv)
        value = own_w[u, :, pl.ds(pl.multiple_of(i * HD, HD), HD)]
        bottom = total * carried + fresh
        for g in range(GROUP):
            span = slice(g * beams, (g + 1) * beams)
            done = (numer[span] * carried[span] + fresh[span] * value) / bottom[span]
            head = pl.ds(pl.multiple_of((i * GROUP + g) * HD, HD), HD)
            out_ref[u, :, head] = done.astype(jnp.bfloat16)

    for c in taken + tables:
        c.start()
    start_fetch(0)
    barrier = pltpu.get_barrier_semaphore()
    for to in peers:
        pl.semaphore_signal(barrier, inc=1, device_id=to, device_id_type=MESH)
    pl.semaphore_wait(barrier, len(peers))

    def send_queries(v, _):
        start(v, *[("z", s) for s in in_z])
        return 0

    for c in taken:
        c.wait()
    own_copy().start()
    lax.fori_loop(0, chunks, send_queries, 0)
    for c in tables:
        c.wait()
    lax.fori_loop(0, users, own_terms, 0)
    own_copy().wait()

    def attend(v):
        @pl.when(v + 1 < chunks)
        def _():
            start_fetch(v + 1)

        gathered(v)
        for c in fetch(v):
            c.wait()
        heads(v, range(cols))
        start(v, ("f",), ("fs",))

    run = dict(
        columns=columns, relay=relay, diagonal=diagonal, attend=attend, paired=paired, crossed=crossed,
        reduced=reduced, finished=finished, delivered=delivered,
    )

    def turn(u, _):
        for name, base, early, late in STEPS:
            def one(v, _, name=name):
                run[name](v)
                return 0

            ends = [upto(chunks, base, early, late, x, jnp) for x in (u - 1, u)]
            lax.fori_loop(*ends, one, 0)
        return 0

    lax.fori_loop(*turns(chunks), turn, 0)

    def close(v, _):
        for name in plan.index:
            make(v, name).wait_send()
        return 0

    lax.fori_loop(0, chunks, close, 0)


def body(queries, key_cache, value_cache, key_table, value_table, lengths, token_ids):
    rows, cols = lax.axis_size("row"), lax.axis_size("col")
    plan = Plan(rows, cols)
    users, beams, _ = queries.shape
    positions = key_cache.shape[1]
    vocab = key_table.shape[0]
    kv = KH // cols
    chunks = users * kv
    lines = GROUP * beams
    lanes = CORES * lines
    outer, inner, planes, half = plan.outer, plan.inner, plan.planes, plan.half
    deep = HD // 2
    f32, bf16 = jnp.float32, jnp.bfloat16
    vmem = pl.BlockSpec(memory_space=pltpu.VMEM)
    hbm = pl.BlockSpec(memory_space=pl.ANY)
    block, stat = (deep, lanes), (2, lanes)

    def numer(*lead):
        return pltpu.VMEM((chunks, *lead, *block), bf16)

    def stats(*lead):
        return pltpu.VMEM((chunks, *lead, *stat), f32)

    x, y = max(inner - 1, 1), max(outer - 1, 1)
    copies = len(plan.index)
    scores = chunks * cols * planes * lanes * positions
    return pl.pallas_call(
        lambda *refs: step_kernel(plan, *refs),
        out_shape=jax.ShapeDtypeStruct(queries.shape, bf16),
        in_specs=[pl.BlockSpec(memory_space=pltpu.SMEM), vmem, hbm, hbm, hbm, hbm, hbm],
        out_specs=vmem,
        scratch_shapes=[
            pltpu.VMEM((chunks, GROUP, beams, HD), bf16),
            pltpu.VMEM((vocab, kv * HD), bf16),
            pltpu.VMEM((vocab, kv * HD), bf16),
            pltpu.VMEM((chunks, lines, 1), f32),
            pltpu.VMEM((users, beams, kv * HD), f32),
            pltpu.VMEM((lanes, HD), f32),
            pltpu.VMEM((lanes, 8), f32),
            pltpu.VMEM((chunks, 8, lanes), f32),
            pltpu.VMEM((chunks, planes, CORES, cols, GROUP, beams, HD), bf16),
            numer(2, planes, cols),
            numer(planes, cols),
            stats(planes, cols),
            stats(planes, cols),
            stats(planes, cols),
            numer(y, x, half),
            stats(y, x, half),
            numer(y, x, cols - half),
            stats(y, x, cols - half),
            numer(x, cols),
            stats(x, cols),
            numer(y, cols),
            stats(y, cols),
            numer(cols - 1),
            stats(cols - 1),
            pltpu.VMEM((chunks, 2, *block), f32),
            pltpu.VMEM((2, cols, positions, HD), bf16),
            pltpu.VMEM((2, cols, positions, HD), bf16),
            pltpu.SemaphoreType.DMA((chunks, copies)),
            pltpu.SemaphoreType.DMA((chunks, copies)),
            pltpu.SemaphoreType.DMA((1 + 4 * cols + chunks * GROUP + 2,)),
        ],
        compiler_params=pltpu.CompilerParams(
            collective_id=0, has_side_effects=True, vmem_limit_bytes=60 * 1024 * 1024
        ),
        cost_estimate=pl.CostEstimate(
            flops=4 * scores * HD, bytes_accessed=4 * key_cache.size, transcendentals=scores
        ),
        name="step",
    )(lengths, token_ids, queries, key_cache, value_cache, key_table, value_table)


def solution(mesh):
    return jax.shard_map(
        body,
        mesh=mesh,
        in_specs=(
            P(None, "row", "col"),
            P(None, ("row", "col"), None),
            P(None, ("row", "col"), None),
            P(),
            P(),
            P(),
            P(None, "row"),
        ),
        out_specs=P(None, "row", "col"),
        check_vma=False,
    )
```

```python
import math

import jax
import jax.numpy as jnp
import numpy as np
from jax import lax
from jax.experimental import pallas as pl
from jax.experimental.pallas import tpu as pltpu
from jax.sharding import PartitionSpec as P

HQ = 32
KH = 8
HD = 128
GROUP = HQ // KH
CORES = 2
LOG2E = math.log2(math.e)
FACTOR = HD ** (-0.5) * LOG2E
MESH = pl.DeviceIdType.MESH
PLANE_FIRST = 3
PLANE_CROSS = 2
PLANE_COLUMNS = 4
STEPS = (
    ("paired", -1, 0, 1),
    ("relay", 4, 0, 2),
    ("columns", 7, 2, 2),
    ("crossed", -7, 4, 1),
    ("diagonal", 2, 0, 4),
    ("attend", 1, 0, 0),
    ("reduced", -8, 2, 2),
    ("delivered", -16, 2, 1),
    ("finished", -14, 4, 1),
)
NEEDS = (
    ("columns", "relay"), ("relay", "diagonal"), ("diagonal", "attend"), ("attend", "paired"), ("paired", "crossed"),
    ("crossed", "reduced"), ("reduced", "finished"), ("finished", "delivered"),
)


def upto(chunks, base, early, late, u, lib):
    some = base + u + lib.minimum(lib.maximum(u, 0), early) + late * lib.maximum(u - (chunks - 1), 0)
    return lib.minimum(lib.maximum(some, 0), chunks)


def turns(chunks):
    first = -max(base for _, base, _, _ in STEPS)
    last, order = first, {}
    while last < chunks or any(upto(chunks, *rest, last - 1, np) < chunks for _, *rest in STEPS):
        for name, *rest in STEPS:
            for v in range(upto(chunks, *rest, last - 1, np), upto(chunks, *rest, last, np)):
                order[name, v] = len(order)
        last += 1
    for before, after in NEEDS:
        assert all(order[before, v] < order[after, v] for v in range(chunks)), (before, after)
    return first, last


class Plan:
    def __init__(self, rows, cols):
        self.rows, self.cols = rows, cols
        self.planes = rows // CORES
        self.outer = 2 if self.planes % 2 == 0 else 1
        self.inner = self.planes // self.outer
        self.half = cols // 2
        names = []
        for s in range(1, cols):
            names += [("z", s), ("zr", s), ("zs", s)]
        for b in range(1, self.inner):
            names += [("bx", b), ("cd", b), ("x", b), ("xs", b)]
        for a in range(1, self.outer):
            names += [("by", a), ("ce", a), ("y", a), ("ys", a)]
            for b in range(1, self.inner):
                names += [(n, a, b) for n in ("ca", "cb", "dd", "ra", "ras", "rb", "rbs")]
        names += [("bd",), ("f",), ("fs",), ("fo",)]
        self.index = {name: at for at, name in enumerate(names)}
        self.same = [n for n in names if n[0] not in ("z", "bx", "by", "bd", "ca", "cb", "cd", "ce", "dd")]
        self.usual = [n for n in names if n not in self.same]
        other = {"z": "pz", "bx": "px", "by": "py", "bd": "pd", "ca": "pca", "cb": "pcb"}
        self.plane = [(other[n[0]], *n[1:]) for n in self.usual if n[0] in other]
        self.index |= {(other[n[0]], *n[1:]): self.index[n] for n in self.usual if n[0] in other}


def step_kernel(
    plan, len_ref, tok_ref, q_hbm, k_hbm, v_hbm, kt_hbm, vt_hbm, out_ref,
    q_in, ktab, vtab, own_e, own_w, turned, turned_st, fin_st,
    q_all, part, from_pair, st, st_pair, sc, ra, ras, rb, rbs, xr, xrs, yr, yrs, zr, zrs, fin,
    kbuf, vbuf, send, recv, local,
):
    chunks = q_in.shape[0]
    outer, inner, cols, half = plan.outer, plan.inner, plan.cols, plan.half
    planes = plan.planes
    kv = KH // cols
    beams = q_in.shape[2]
    lines = GROUP * beams
    lanes = CORES * lines
    positions = k_hbm.shape[1]
    users = k_hbm.shape[0]
    vocab = ktab.shape[0]
    row, col = lax.axis_index("row"), lax.axis_index("col")
    k = lax.rem(row, CORES)
    pair = 1 - k
    me = row // CORES
    b_at, a_at = lax.rem(me, inner), me // inner
    offset = (row * cols + col) * positions

    def spot(a=0, b=0):
        return lax.rem(a_at + a + outer, outer) * inner + lax.rem(b_at + b + inner, inner)

    def at_spot(a=0, b=0):
        return {"row": spot(a, b) * CORES + k}

    def at_col(s):
        return {"col": lax.rem(col + s, cols)}

    at_pair = {"row": me * CORES + pair}
    in_x = range(1, inner)
    in_y = range(1, outer)
    in_xy = [(a, b) for a in in_y for b in in_x]
    in_z = range(1, cols)

    peers = [at_pair] + [at_col(s) for s in in_z] + [at_spot(0, b) for b in in_x] + [at_spot(a, 0) for a in in_y]

    def copy(v, name, src, dst, to):
        at = plan.index[name]
        return pltpu.make_async_remote_copy(
            src_ref=src, dst_ref=dst, send_sem=send.at[v, at], recv_sem=recv.at[v, at],
            device_id=to, device_id_type=MESH,
        )

    low, high = pl.ds(0, half), pl.ds(half, cols - half)
    first_groups, last_groups = pl.ds(0, GROUP // 2), pl.ds(GROUP // 2, GROUP - GROUP // 2)
    turned_at = chunks - min(PLANE_FIRST, chunks // 4)

    def make(v, name):
        kind, *at = name
        if kind == "z":
            return copy(v, name, q_in.at[v], q_all.at[v, me, k, col], at_col(at[0]))
        if kind in ("bx", "by", "bd"):
            to = at_pair if kind == "bd" else at_spot(0, at[0]) if kind == "bx" else at_spot(at[0], 0)
            own = q_all.at[v, me, k]
            return copy(v, name, own, own, to)
        if kind in ("px", "py"):
            own = q_all.at[v, me, k, col]
            return copy(v, name, own, own, at_spot(0, at[0]) if kind == "px" else at_spot(at[0], 0))
        if kind == "pca":
            ref = q_all.at[v, spot(0, -at[1]), k, col, first_groups]
            return copy(v, name, ref, ref, at_spot(at[0], 0))
        if kind == "pcb":
            ref = q_all.at[v, spot(-at[0], 0), k, col, last_groups]
            return copy(v, name, ref, ref, at_spot(0, at[1]))
        if kind == "pz":
            ref = q_all.at[v, :, k, col]
            return copy(v, name, ref, ref, at_col(at[0]))
        if kind == "pd":
            ref = q_all.at[v, :, k]
            return copy(v, name, ref, ref, at_pair)
        if kind == "cd":
            ref = q_all.at[v, spot(0, -at[0]), k]
            return copy(v, name, ref, ref, at_pair)
        if kind == "ce":
            ref = q_all.at[v, spot(-at[0], 0), k]
            return copy(v, name, ref, ref, at_pair)
        if kind == "ca":
            ref = q_all.at[v, spot(0, -at[1]), k, low]
            return copy(v, name, ref, ref, at_spot(at[0], 0))
        if kind == "cb":
            ref = q_all.at[v, spot(-at[0], 0), k, high]
            return copy(v, name, ref, ref, at_spot(0, at[1]))
        if kind == "dd":
            ref = q_all.at[v, spot(-at[0], -at[1]), k]
            return copy(v, name, ref, ref, at_pair)
        if kind == "f":
            return copy(v, name, part.at[v, pair], from_pair.at[v], at_pair)
        if kind == "fs":
            return copy(v, name, st.at[v], st_pair.at[v], at_pair)
        if kind == "ra":
            return copy(v, name, part.at[v, k, spot(*at), low], ra.at[v, at[0] - 1, at[1] - 1], at_spot(at[0], 0))
        if kind == "ras":
            return copy(v, name, sc.at[v, spot(*at), low], ras.at[v, at[0] - 1, at[1] - 1], at_spot(at[0], 0))
        if kind == "rb":
            return copy(v, name, part.at[v, k, spot(*at), high], rb.at[v, at[0] - 1, at[1] - 1], at_spot(0, at[1]))
        if kind == "rbs":
            return copy(v, name, sc.at[v, spot(*at), high], rbs.at[v, at[0] - 1, at[1] - 1], at_spot(0, at[1]))
        if kind == "x":
            return copy(v, name, part.at[v, k, spot(0, at[0])], xr.at[v, at[0] - 1], at_spot(0, at[0]))
        if kind == "xs":
            return copy(v, name, sc.at[v, spot(0, at[0])], xrs.at[v, at[0] - 1], at_spot(0, at[0]))
        if kind == "y":
            return copy(v, name, part.at[v, k, spot(at[0], 0)], yr.at[v, at[0] - 1], at_spot(at[0], 0))
        if kind == "ys":
            return copy(v, name, sc.at[v, spot(at[0], 0)], yrs.at[v, at[0] - 1], at_spot(at[0], 0))
        if kind == "zr":
            there = lax.rem(col + at[0], cols)
            return copy(v, name, part.at[v, k, me, there], zr.at[v, at[0] - 1], at_col(at[0]))
        if kind == "zs":
            there = lax.rem(col + at[0], cols)
            return copy(v, name, sc.at[v, me, there], zrs.at[v, at[0] - 1], at_col(at[0]))
        return copy(v, name, fin.at[v, k], fin.at[v, k], at_pair)

    def start(v, *names):
        for name in names:
            make(v, name).start()

    def arrived(v, *names):
        for name in names:
            make(v, name).wait_recv()

    def own_copy():
        return pltpu.make_async_copy(q_in, q_all.at[:, me, k, col], local.at[0])

    spare = 1 + 4 * cols
    wide = pl.ds(pl.multiple_of(col * kv * HD, HD), kv * HD)
    taken = [
        pltpu.make_async_copy(
            q_hbm.at[u, :, pl.ds((i * GROUP + g) * HD, HD)],
            q_in.at[u * kv + i, g],
            local.at[spare + (u * kv + i) * GROUP + g],
        )
        for u in range(users)
        for i in range(kv)
        for g in range(GROUP)
    ]
    spare += len(taken)
    tables = [
        pltpu.make_async_copy(kt_hbm.at[:, wide], ktab, local.at[spare]),
        pltpu.make_async_copy(vt_hbm.at[:, wide], vtab, local.at[spare + 1]),
    ]

    def own_terms(u, _):
        pick = lax.broadcasted_iota(jnp.int32, (vocab, beams), 0) == tok_ref[pl.ds(u, 1), :]
        pick = jnp.where(pick, 1.0, 0.0).astype(jnp.bfloat16)
        found, own_w[u] = (
            lax.dot_general(pick, tab[...], (((0,), (0,)), ((), ())), preferred_element_type=jnp.float32)
            for tab in (ktab, vtab)
        )
        for i in range(kv):
            keys = found[:, i * HD : (i + 1) * HD]
            for g in range(GROUP):
                q = q_in[u * kv + i, g].astype(jnp.float32)
                own_e[u * kv + i, g * beams : (g + 1) * beams] = jnp.sum(q * keys, axis=1, keepdims=True) * FACTOR
        return 0

    def fetch(v):
        slot = lax.rem(v, 2)
        found = []
        for c in range(cols):
            at = pl.ds(pl.multiple_of((c * kv + lax.rem(v, kv)) * HD, HD), HD)
            for n, (src, dst) in enumerate([(k_hbm, kbuf), (v_hbm, vbuf)]):
                found.append(
                    pltpu.make_async_copy(src.at[v // kv, :, at], dst.at[slot, c], local.at[1 + (c * 2 + n) * 2 + slot])
                )
        return found

    def start_fetch(v):
        for c in fetch(v):
            c.start()

    def either(v, usual, plane):
        pl.when(v < turned_at)(usual)
        pl.when(v >= turned_at)(plane)

    def plane_cross(v):
        for b in in_x:
            arrived(v, ("px", b))
            start(v, *[("pca", a, b) for a in in_y])
        for a in in_y:
            arrived(v, ("py", a))
            start(v, *[("pcb", a, b) for b in in_x])

    def plane_columns(v):
        for a, b in in_xy:
            arrived(v, ("pca", a, b), ("pcb", a, b))
        start(v, *[("pz", s) for s in in_z])

    def columns(v):
        @pl.when(v < turned_at)
        def _():
            arrived(v, *[("z", s) for s in in_z])
            start(v, *[("bx", b) for b in in_x], *[("by", a) for a in in_y], ("bd",))

    def relay(v):
        @pl.when(v < turned_at)
        def _():
            for b in in_x:
                arrived(v, ("bx", b))
                start(v, *[("ca", a, b) for a in in_y], ("cd", b))
            for a in in_y:
                arrived(v, ("by", a))
                start(v, *[("cb", a, b) for b in in_x], ("ce", a))

    def diagonal(v):
        def usual():
            for a, b in in_xy:
                arrived(v, ("ca", a, b), ("cb", a, b))
                start(v, ("dd", a, b))

        def plane():
            arrived(v, *[("pz", s) for s in in_z])
            start(v, ("pd",))

        either(v, usual, plane)

    def gathered(v):
        def usual():
            arrived(v, ("bd",), *[("cd", b) for b in in_x], *[("ce", a) for a in in_y])
            arrived(v, *[("dd", a, b) for a, b in in_xy])

        either(v, usual, lambda: arrived(v, ("pd",)))

    def heads(v, some):
        slot = lax.rem(v, 2)
        keep = lax.broadcasted_iota(jnp.int32, (positions, planes * lanes), 0) < len_ref[v // kv] - offset
        for c in some:
            q = q_all[v, :, :, c].reshape(planes * lanes, HD)
            s = lax.dot_general(kbuf[slot, c], q, (((1,), (1,)), ((), ())), preferred_element_type=jnp.float32)
            s = jnp.where(keep, s, -1e30)
            m = jnp.max(s, axis=0, keepdims=True)
            p = jnp.exp2((s - m) * FACTOR)
            total = jnp.sum(p, axis=0, keepdims=True)
            m = m * FACTOR
            o = lax.dot_general(
                vbuf[slot, c], p.astype(jnp.bfloat16), (((0,), (0,)), ((), ())), preferred_element_type=jnp.float32
            ).astype(jnp.bfloat16)
            for at in range(planes):
                span = slice(at * lanes, (at + 1) * lanes)
                st[v, at, c, :1, :] = m[:, span]
                st[v, at, c, 1:, :] = total[:, span]
                for h in range(2):
                    part[v, h, at, c] = o[h * (HD // 2) : (h + 1) * (HD // 2), span]

    def fuse(numers, stats):
        peaks = [x[..., :1, :] for x in stats]
        peak = peaks[0]
        for x in peaks[1:]:
            peak = jnp.maximum(peak, x)
        scales = [jnp.exp2(x - peak) for x in peaks]
        total = sum(x[..., 1:, :] * scale for x, scale in zip(stats, scales))
        numer = sum(x.astype(jnp.float32) * scale for x, scale in zip(numers, scales))
        return numer, peak, total

    def put(v, at, span, numer, peak, total):
        part[v, k, at, span] = numer.astype(jnp.bfloat16)
        sc[v, at, span, :1, :] = peak
        sc[v, at, span, 1:, :] = total

    def fuse_into(v, at, span, numers, stats):
        put(v, at, span, *fuse([part[v, k, at, span]] + numers, [sc[v, at, span]] + stats))

    def paired(v):
        arrived(v, ("f",), ("fs",))
        for at in range(planes):
            put(
                v, at, pl.ds(0, cols),
                *fuse([part[v, k, at], from_pair[v, at]], [st[v, at], st_pair[v, at]]),
            )
        for a, b in in_xy:
            start(v, ("ra", a, b), ("ras", a, b), ("rb", a, b), ("rbs", a, b))

    def crossed(v):
        for a, b in in_xy:
            arrived(v, ("ra", a, b), ("ras", a, b), ("rb", a, b), ("rbs", a, b))
        if in_xy:
            for b in in_x:
                fuse_into(
                    v, spot(0, b), low,
                    [ra[v, a - 1, b - 1] for a in in_y], [ras[v, a - 1, b - 1] for a in in_y],
                )
            for a in in_y:
                fuse_into(
                    v, spot(a, 0), high,
                    [rb[v, a - 1, b - 1] for b in in_x], [rbs[v, a - 1, b - 1] for b in in_x],
                )
        for b in in_x:
            start(v, ("x", b), ("xs", b))
        for a in in_y:
            start(v, ("y", a), ("ys", a))

    def reduced(v):
        for b in in_x:
            arrived(v, ("x", b), ("xs", b))
        for a in in_y:
            arrived(v, ("y", a), ("ys", a))
        fuse_into(
            v, me, pl.ds(0, cols),
            [xr[v, b - 1] for b in in_x] + [yr[v, a - 1] for a in in_y],
            [xrs[v, b - 1] for b in in_x] + [yrs[v, a - 1] for a in in_y],
        )
        for s in in_z:
            start(v, ("zr", s), ("zs", s))

    def finished(v):
        for s in in_z:
            arrived(v, ("zr", s), ("zs", s))
        numer, peak, total = fuse(
            [part[v, k, me, col]] + [zr[v, s - 1] for s in in_z],
            [sc[v, me, col]] + [zrs[v, s - 1] for s in in_z],
        )
        fin[v, k] = numer
        fin_st[v, :1] = peak
        fin_st[v, 1:2] = total
        start(v, ("fo",))

    def delivered(v):
        arrived(v, ("fo",))
        turned[...] = fin[v].reshape(HD, lanes).T
        turned_st[...] = fin_st[v].T
        mine = pl.ds(pl.multiple_of(k * lines, lines), lines)
        numer = turned[mine, :]
        peak, total = turned_st[mine, 0:1], turned_st[mine, 1:2]
        own = own_e[v]
        top = jnp.maximum(peak, own)
        carried, fresh = jnp.exp2(peak - top), jnp.exp2(own - top)
        u, i = v // kv, lax.rem(v, kv)
        value = own_w[u, :, pl.ds(pl.multiple_of(i * HD, HD), HD)]
        bottom = total * carried + fresh
        for g in range(GROUP):
            span = slice(g * beams, (g + 1) * beams)
            done = (numer[span] * carried[span] + fresh[span] * value) / bottom[span]
            head = pl.ds(pl.multiple_of((i * GROUP + g) * HD, HD), HD)
            out_ref[u, :, head] = done.astype(jnp.bfloat16)

    for c in taken + tables:
        c.start()
    start_fetch(0)
    barrier = pltpu.get_barrier_semaphore()
    for to in peers:
        pl.semaphore_signal(barrier, inc=1, device_id=to, device_id_type=MESH)
    pl.semaphore_wait(barrier, len(peers))

    def send_queries(v, _):
        start(v, *[("z", s) for s in in_z])
        return 0

    for c in taken:
        c.wait()
    own_copy().start()
    lax.fori_loop(0, turned_at, send_queries, 0)
    own_copy().wait()

    def send_plane(v, _):
        start(v, *[("px", b) for b in in_x], *[("py", a) for a in in_y])
        return 0

    lax.fori_loop(turned_at, chunks, send_plane, 0)
    for c in tables:
        c.wait()
    lax.fori_loop(0, users, own_terms, 0)

    def attend(v):
        @pl.when(v + 1 < chunks)
        def _():
            start_fetch(v + 1)

        gathered(v)
        for c in fetch(v):
            c.wait()
        heads(v, range(cols))
        start(v, ("f",), ("fs",))

    run = dict(
        columns=columns, relay=relay, diagonal=diagonal, attend=attend, paired=paired, crossed=crossed,
        reduced=reduced, finished=finished, delivered=delivered,
    )

    begin, end = turns(chunks)

    def each(step):
        def one(v, _):
            step(v)
            return 0

        lax.fori_loop(turned_at, chunks, one, 0)

    def turn(u, _):
        pl.when(u == begin + PLANE_CROSS)(lambda: each(plane_cross))
        pl.when(u == begin + PLANE_COLUMNS)(lambda: each(plane_columns))
        for name, base, early, late in STEPS:
            def one(v, _, name=name):
                run[name](v)
                return 0

            ends = [upto(chunks, base, early, late, x, jnp) for x in (u - 1, u)]
            lax.fori_loop(*ends, one, 0)
        return 0

    lax.fori_loop(begin, end, turn, 0)

    def close(v, _):
        def sent(names):
            for name in names:
                make(v, name).wait_send()

        sent(plan.same)
        either(v, lambda: sent(plan.usual), lambda: sent(plan.plane))
        return 0

    lax.fori_loop(0, chunks, close, 0)


def body(queries, key_cache, value_cache, key_table, value_table, lengths, token_ids):
    rows, cols = lax.axis_size("row"), lax.axis_size("col")
    plan = Plan(rows, cols)
    users, beams, _ = queries.shape
    positions = key_cache.shape[1]
    vocab = key_table.shape[0]
    kv = KH // cols
    chunks = users * kv
    lines = GROUP * beams
    lanes = CORES * lines
    outer, inner, planes, half = plan.outer, plan.inner, plan.planes, plan.half
    deep = HD // 2
    f32, bf16 = jnp.float32, jnp.bfloat16
    vmem = pl.BlockSpec(memory_space=pltpu.VMEM)
    hbm = pl.BlockSpec(memory_space=pl.ANY)
    block, stat = (deep, lanes), (2, lanes)

    def numer(*lead):
        return pltpu.VMEM((chunks, *lead, *block), bf16)

    def stats(*lead):
        return pltpu.VMEM((chunks, *lead, *stat), f32)

    x, y = max(inner - 1, 1), max(outer - 1, 1)
    copies = len(plan.same + plan.usual)
    scores = chunks * cols * planes * lanes * positions
    return pl.pallas_call(
        lambda *refs: step_kernel(plan, *refs),
        out_shape=jax.ShapeDtypeStruct(queries.shape, bf16),
        in_specs=[pl.BlockSpec(memory_space=pltpu.SMEM), vmem, hbm, hbm, hbm, hbm, hbm],
        out_specs=vmem,
        scratch_shapes=[
            pltpu.VMEM((chunks, GROUP, beams, HD), bf16),
            pltpu.VMEM((vocab, kv * HD), bf16),
            pltpu.VMEM((vocab, kv * HD), bf16),
            pltpu.VMEM((chunks, lines, 1), f32),
            pltpu.VMEM((users, beams, kv * HD), f32),
            pltpu.VMEM((lanes, HD), f32),
            pltpu.VMEM((lanes, 8), f32),
            pltpu.VMEM((chunks, 8, lanes), f32),
            pltpu.VMEM((chunks, planes, CORES, cols, GROUP, beams, HD), bf16),
            numer(2, planes, cols),
            numer(planes, cols),
            stats(planes, cols),
            stats(planes, cols),
            stats(planes, cols),
            numer(y, x, half),
            stats(y, x, half),
            numer(y, x, cols - half),
            stats(y, x, cols - half),
            numer(x, cols),
            stats(x, cols),
            numer(y, cols),
            stats(y, cols),
            numer(cols - 1),
            stats(cols - 1),
            pltpu.VMEM((chunks, 2, *block), f32),
            pltpu.VMEM((2, cols, positions, HD), bf16),
            pltpu.VMEM((2, cols, positions, HD), bf16),
            pltpu.SemaphoreType.DMA((chunks, copies)),
            pltpu.SemaphoreType.DMA((chunks, copies)),
            pltpu.SemaphoreType.DMA((1 + 4 * cols + chunks * GROUP + 2,)),
        ],
        compiler_params=pltpu.CompilerParams(
            collective_id=0, has_side_effects=True, vmem_limit_bytes=60 * 1024 * 1024
        ),
        cost_estimate=pl.CostEstimate(
            flops=4 * scores * HD, bytes_accessed=4 * key_cache.size, transcendentals=scores
        ),
        name="step",
    )(lengths, token_ids, queries, key_cache, value_cache, key_table, value_table)


def solution(mesh):
    return jax.shard_map(
        body,
        mesh=mesh,
        in_specs=(
            P(None, "row", "col"),
            P(None, ("row", "col"), None),
            P(None, ("row", "col"), None),
            P(),
            P(),
            P(),
            P(None, "row"),
        ),
        out_specs=P(None, "row", "col"),
        check_vma=False,
    )
```

```python
import math

import jax
import jax.numpy as jnp
import numpy as np
from jax import lax
from jax.experimental import pallas as pl
from jax.experimental.pallas import tpu as pltpu
from jax.sharding import PartitionSpec as P

HQ = 32
KH = 8
HD = 128
GROUP = HQ // KH
CORES = 2
LOG2E = math.log2(math.e)
FACTOR = HD ** (-0.5) * LOG2E
MESH = pl.DeviceIdType.MESH
PLANE_FIRST = 4
PLANE_CROSS = 2
PLANE_COLUMNS = 4
STEPS = (
    ("paired", -1, 0, 1),
    ("relay", 4, 0, 2),
    ("columns", 7, 2, 2),
    ("crossed", -7, 4, 1),
    ("diagonal", 2, 0, 4),
    ("attend", 1, 0, 0),
    ("reduced", -8, 2, 2),
    ("delivered", -16, 2, 1),
    ("finished", -14, 4, 1),
)
NEEDS = (
    ("columns", "relay"), ("relay", "diagonal"), ("diagonal", "attend"), ("attend", "paired"), ("paired", "crossed"),
    ("crossed", "reduced"), ("reduced", "finished"), ("finished", "delivered"),
)


def upto(chunks, base, early, late, u, lib):
    some = base + u + lib.minimum(lib.maximum(u, 0), early) + late * lib.maximum(u - (chunks - 1), 0)
    return lib.minimum(lib.maximum(some, 0), chunks)


def turns(chunks):
    first = -max(base for _, base, _, _ in STEPS)
    last, order = first, {}
    while last < chunks or any(upto(chunks, *rest, last - 1, np) < chunks for _, *rest in STEPS):
        for name, *rest in STEPS:
            for v in range(upto(chunks, *rest, last - 1, np), upto(chunks, *rest, last, np)):
                order[name, v] = len(order)
        last += 1
    for before, after in NEEDS:
        assert all(order[before, v] < order[after, v] for v in range(chunks)), (before, after)
    return first, last


class Plan:
    def __init__(self, rows, cols):
        self.rows, self.cols = rows, cols
        self.planes = rows // CORES
        self.outer = 2 if self.planes % 2 == 0 else 1
        self.inner = self.planes // self.outer
        self.half = cols // 2
        names = []
        for s in range(1, cols):
            names += [("z", s), ("zr", s), ("zs", s)]
        for b in range(1, self.inner):
            names += [("bx", b), ("cd", b), ("x", b), ("xs", b)]
        for a in range(1, self.outer):
            names += [("by", a), ("ce", a), ("y", a), ("ys", a)]
            for b in range(1, self.inner):
                names += [(n, a, b) for n in ("ca", "cb", "dd", "ra", "ras", "rb", "rbs")]
        names += [("bd",), ("f",), ("fs",), ("fo",)]
        self.index = {name: at for at, name in enumerate(names)}
        self.same = [n for n in names if n[0] not in ("z", "bx", "by", "bd", "ca", "cb", "cd", "ce", "dd")]
        self.usual = [n for n in names if n not in self.same]
        other = {"z": "pz", "bx": "px", "by": "py", "bd": "pd", "ca": "pca", "cb": "pcb"}
        self.plane = [(other[n[0]], *n[1:]) for n in self.usual if n[0] in other]
        self.index |= {(other[n[0]], *n[1:]): self.index[n] for n in self.usual if n[0] in other}


def step_kernel(
    plan, len_ref, tok_ref, q_hbm, k_hbm, v_hbm, kt_hbm, vt_hbm, out_ref,
    q_in, ktab, vtab, own_e, own_w, turned, turned_st, fin_st,
    q_all, part, from_pair, st, st_pair, sc, ra, ras, rb, rbs, xr, xrs, yr, yrs, zr, zrs, fin,
    kbuf, vbuf, send, recv, local,
):
    chunks = q_in.shape[0]
    outer, inner, cols, half = plan.outer, plan.inner, plan.cols, plan.half
    planes = plan.planes
    kv = KH // cols
    beams = q_in.shape[2]
    lines = GROUP * beams
    lanes = CORES * lines
    positions = k_hbm.shape[1]
    users = k_hbm.shape[0]
    vocab = ktab.shape[0]
    row, col = lax.axis_index("row"), lax.axis_index("col")
    k = lax.rem(row, CORES)
    pair = 1 - k
    me = row // CORES
    b_at, a_at = lax.rem(me, inner), me // inner
    offset = (row * cols + col) * positions

    def spot(a=0, b=0):
        return lax.rem(a_at + a + outer, outer) * inner + lax.rem(b_at + b + inner, inner)

    def at_spot(a=0, b=0):
        return {"row": spot(a, b) * CORES + k}

    def at_col(s):
        return {"col": lax.rem(col + s, cols)}

    at_pair = {"row": me * CORES + pair}
    in_x = range(1, inner)
    in_y = range(1, outer)
    in_xy = [(a, b) for a in in_y for b in in_x]
    in_z = range(1, cols)

    peers = [at_pair] + [at_col(s) for s in in_z] + [at_spot(0, b) for b in in_x] + [at_spot(a, 0) for a in in_y]

    def copy(v, name, src, dst, to):
        at = plan.index[name]
        return pltpu.make_async_remote_copy(
            src_ref=src, dst_ref=dst, send_sem=send.at[v, at], recv_sem=recv.at[v, at],
            device_id=to, device_id_type=MESH,
        )

    low, high = pl.ds(0, half), pl.ds(half, cols - half)
    first_groups, last_groups = pl.ds(0, GROUP // 2), pl.ds(GROUP // 2, GROUP - GROUP // 2)
    turned_at = chunks - min(PLANE_FIRST, chunks // 4)

    def make(v, name):
        kind, *at = name
        if kind == "z":
            return copy(v, name, q_in.at[v], q_all.at[v, me, k, col], at_col(at[0]))
        if kind in ("bx", "by", "bd"):
            to = at_pair if kind == "bd" else at_spot(0, at[0]) if kind == "bx" else at_spot(at[0], 0)
            own = q_all.at[v, me, k]
            return copy(v, name, own, own, to)
        if kind in ("px", "py"):
            own = q_all.at[v, me, k, col]
            return copy(v, name, own, own, at_spot(0, at[0]) if kind == "px" else at_spot(at[0], 0))
        if kind == "pca":
            ref = q_all.at[v, spot(0, -at[1]), k, col, first_groups]
            return copy(v, name, ref, ref, at_spot(at[0], 0))
        if kind == "pcb":
            ref = q_all.at[v, spot(-at[0], 0), k, col, last_groups]
            return copy(v, name, ref, ref, at_spot(0, at[1]))
        if kind == "pz":
            ref = q_all.at[v, :, k, col]
            return copy(v, name, ref, ref, at_col(at[0]))
        if kind == "pd":
            ref = q_all.at[v, :, k]
            return copy(v, name, ref, ref, at_pair)
        if kind == "cd":
            ref = q_all.at[v, spot(0, -at[0]), k]
            return copy(v, name, ref, ref, at_pair)
        if kind == "ce":
            ref = q_all.at[v, spot(-at[0], 0), k]
            return copy(v, name, ref, ref, at_pair)
        if kind == "ca":
            ref = q_all.at[v, spot(0, -at[1]), k, low]
            return copy(v, name, ref, ref, at_spot(at[0], 0))
        if kind == "cb":
            ref = q_all.at[v, spot(-at[0], 0), k, high]
            return copy(v, name, ref, ref, at_spot(0, at[1]))
        if kind == "dd":
            ref = q_all.at[v, spot(-at[0], -at[1]), k]
            return copy(v, name, ref, ref, at_pair)
        if kind == "f":
            return copy(v, name, part.at[v, pair], from_pair.at[v], at_pair)
        if kind == "fs":
            return copy(v, name, st.at[v], st_pair.at[v], at_pair)
        if kind == "ra":
            return copy(v, name, part.at[v, k, spot(*at), low], ra.at[v, at[0] - 1, at[1] - 1], at_spot(at[0], 0))
        if kind == "ras":
            return copy(v, name, sc.at[v, spot(*at), low], ras.at[v, at[0] - 1, at[1] - 1], at_spot(at[0], 0))
        if kind == "rb":
            return copy(v, name, part.at[v, k, spot(*at), high], rb.at[v, at[0] - 1, at[1] - 1], at_spot(0, at[1]))
        if kind == "rbs":
            return copy(v, name, sc.at[v, spot(*at), high], rbs.at[v, at[0] - 1, at[1] - 1], at_spot(0, at[1]))
        if kind == "x":
            return copy(v, name, part.at[v, k, spot(0, at[0])], xr.at[v, at[0] - 1], at_spot(0, at[0]))
        if kind == "xs":
            return copy(v, name, sc.at[v, spot(0, at[0])], xrs.at[v, at[0] - 1], at_spot(0, at[0]))
        if kind == "y":
            return copy(v, name, part.at[v, k, spot(at[0], 0)], yr.at[v, at[0] - 1], at_spot(at[0], 0))
        if kind == "ys":
            return copy(v, name, sc.at[v, spot(at[0], 0)], yrs.at[v, at[0] - 1], at_spot(at[0], 0))
        if kind == "zr":
            there = lax.rem(col + at[0], cols)
            return copy(v, name, part.at[v, k, me, there], zr.at[v, at[0] - 1], at_col(at[0]))
        if kind == "zs":
            there = lax.rem(col + at[0], cols)
            return copy(v, name, sc.at[v, me, there], zrs.at[v, at[0] - 1], at_col(at[0]))
        return copy(v, name, fin.at[v, k], fin.at[v, k], at_pair)

    def start(v, *names):
        for name in names:
            make(v, name).start()

    def arrived(v, *names):
        for name in names:
            make(v, name).wait_recv()

    def own_copy():
        return pltpu.make_async_copy(q_in, q_all.at[:, me, k, col], local.at[0])

    spare = 1 + 4 * cols
    wide = pl.ds(pl.multiple_of(col * kv * HD, HD), kv * HD)
    taken = [
        pltpu.make_async_copy(
            q_hbm.at[u, :, pl.ds((i * GROUP + g) * HD, HD)],
            q_in.at[u * kv + i, g],
            local.at[spare + (u * kv + i) * GROUP + g],
        )
        for u in range(users)
        for i in range(kv)
        for g in range(GROUP)
    ]
    spare += len(taken)
    tables = [
        pltpu.make_async_copy(kt_hbm.at[:, wide], ktab, local.at[spare]),
        pltpu.make_async_copy(vt_hbm.at[:, wide], vtab, local.at[spare + 1]),
    ]

    def own_terms(u, _):
        pick = lax.broadcasted_iota(jnp.int32, (vocab, beams), 0) == tok_ref[pl.ds(u, 1), :]
        pick = jnp.where(pick, 1.0, 0.0).astype(jnp.bfloat16)
        found, own_w[u] = (
            lax.dot_general(pick, tab[...], (((0,), (0,)), ((), ())), preferred_element_type=jnp.float32)
            for tab in (ktab, vtab)
        )
        for i in range(kv):
            keys = found[:, i * HD : (i + 1) * HD]
            for g in range(GROUP):
                q = q_in[u * kv + i, g].astype(jnp.float32)
                own_e[u * kv + i, g * beams : (g + 1) * beams] = jnp.sum(q * keys, axis=1, keepdims=True) * FACTOR
        return 0

    def fetch(v):
        slot = lax.rem(v, 2)
        found = []
        for c in range(cols):
            at = pl.ds(pl.multiple_of((c * kv + lax.rem(v, kv)) * HD, HD), HD)
            for n, (src, dst) in enumerate([(k_hbm, kbuf), (v_hbm, vbuf)]):
                found.append(
                    pltpu.make_async_copy(src.at[v // kv, :, at], dst.at[slot, c], local.at[1 + (c * 2 + n) * 2 + slot])
                )
        return found

    def start_fetch(v):
        for c in fetch(v):
            c.start()

    def either(v, usual, plane):
        pl.when(v < turned_at)(usual)
        pl.when(v >= turned_at)(plane)

    def plane_cross(v):
        for b in in_x:
            arrived(v, ("px", b))
            start(v, *[("pca", a, b) for a in in_y])
        for a in in_y:
            arrived(v, ("py", a))
            start(v, *[("pcb", a, b) for b in in_x])

    def plane_columns(v):
        for a, b in in_xy:
            arrived(v, ("pca", a, b), ("pcb", a, b))
        start(v, *[("pz", s) for s in in_z])

    def columns(v):
        @pl.when(v < turned_at)
        def _():
            arrived(v, *[("z", s) for s in in_z])
            start(v, *[("bx", b) for b in in_x], *[("by", a) for a in in_y], ("bd",))

    def relay(v):
        @pl.when(v < turned_at)
        def _():
            for b in in_x:
                arrived(v, ("bx", b))
                start(v, *[("ca", a, b) for a in in_y], ("cd", b))
            for a in in_y:
                arrived(v, ("by", a))
                start(v, *[("cb", a, b) for b in in_x], ("ce", a))

    def diagonal(v):
        def usual():
            for a, b in in_xy:
                arrived(v, ("ca", a, b), ("cb", a, b))
                start(v, ("dd", a, b))

        def plane():
            arrived(v, *[("pz", s) for s in in_z])
            start(v, ("pd",))

        either(v, usual, plane)

    def gathered(v):
        def usual():
            arrived(v, ("bd",), *[("cd", b) for b in in_x], *[("ce", a) for a in in_y])
            arrived(v, *[("dd", a, b) for a, b in in_xy])

        either(v, usual, lambda: arrived(v, ("pd",)))

    def heads(v, some):
        slot = lax.rem(v, 2)
        keep = lax.broadcasted_iota(jnp.int32, (positions, planes * lanes), 0) < len_ref[v // kv] - offset
        for c in some:
            q = q_all[v, :, :, c].reshape(planes * lanes, HD)
            s = lax.dot_general(kbuf[slot, c], q, (((1,), (1,)), ((), ())), preferred_element_type=jnp.float32)
            s = jnp.where(keep, s, -1e30)
            m = jnp.max(s, axis=0, keepdims=True)
            p = jnp.exp2((s - m) * FACTOR)
            total = jnp.sum(p, axis=0, keepdims=True)
            m = m * FACTOR
            o = lax.dot_general(
                vbuf[slot, c], p.astype(jnp.bfloat16), (((0,), (0,)), ((), ())), preferred_element_type=jnp.float32
            ).astype(jnp.bfloat16)
            for at in range(planes):
                span = slice(at * lanes, (at + 1) * lanes)
                st[v, at, c, :1, :] = m[:, span]
                st[v, at, c, 1:, :] = total[:, span]
                for h in range(2):
                    part[v, h, at, c] = o[h * (HD // 2) : (h + 1) * (HD // 2), span]

    def fuse(numers, stats):
        peaks = [x[..., :1, :] for x in stats]
        peak = peaks[0]
        for x in peaks[1:]:
            peak = jnp.maximum(peak, x)
        scales = [jnp.exp2(x - peak) for x in peaks]
        total = sum(x[..., 1:, :] * scale for x, scale in zip(stats, scales))
        numer = sum(x.astype(jnp.float32) * scale for x, scale in zip(numers, scales))
        return numer, peak, total

    def put(v, at, span, numer, peak, total):
        part[v, k, at, span] = numer.astype(jnp.bfloat16)
        sc[v, at, span, :1, :] = peak
        sc[v, at, span, 1:, :] = total

    def fuse_into(v, at, span, numers, stats):
        put(v, at, span, *fuse([part[v, k, at, span]] + numers, [sc[v, at, span]] + stats))

    def paired(v):
        arrived(v, ("f",), ("fs",))
        for at in range(planes):
            put(
                v, at, pl.ds(0, cols),
                *fuse([part[v, k, at], from_pair[v, at]], [st[v, at], st_pair[v, at]]),
            )
        for a, b in in_xy:
            start(v, ("ra", a, b), ("ras", a, b), ("rb", a, b), ("rbs", a, b))

    def crossed(v):
        for a, b in in_xy:
            arrived(v, ("ra", a, b), ("ras", a, b), ("rb", a, b), ("rbs", a, b))
        if in_xy:
            for b in in_x:
                fuse_into(
                    v, spot(0, b), low,
                    [ra[v, a - 1, b - 1] for a in in_y], [ras[v, a - 1, b - 1] for a in in_y],
                )
            for a in in_y:
                fuse_into(
                    v, spot(a, 0), high,
                    [rb[v, a - 1, b - 1] for b in in_x], [rbs[v, a - 1, b - 1] for b in in_x],
                )
        for b in in_x:
            start(v, ("x", b), ("xs", b))
        for a in in_y:
            start(v, ("y", a), ("ys", a))

    def reduced(v):
        for b in in_x:
            arrived(v, ("x", b), ("xs", b))
        for a in in_y:
            arrived(v, ("y", a), ("ys", a))
        fuse_into(
            v, me, pl.ds(0, cols),
            [xr[v, b - 1] for b in in_x] + [yr[v, a - 1] for a in in_y],
            [xrs[v, b - 1] for b in in_x] + [yrs[v, a - 1] for a in in_y],
        )
        for s in in_z:
            start(v, ("zr", s), ("zs", s))

    def finished(v):
        for s in in_z:
            arrived(v, ("zr", s), ("zs", s))
        numer, peak, total = fuse(
            [part[v, k, me, col]] + [zr[v, s - 1] for s in in_z],
            [sc[v, me, col]] + [zrs[v, s - 1] for s in in_z],
        )
        fin[v, k] = numer
        fin_st[v, :1] = peak
        fin_st[v, 1:2] = total
        start(v, ("fo",))

    def delivered(v):
        arrived(v, ("fo",))
        turned[...] = fin[v].reshape(HD, lanes).T
        turned_st[...] = fin_st[v].T
        mine = pl.ds(pl.multiple_of(k * lines, lines), lines)
        numer = turned[mine, :]
        peak, total = turned_st[mine, 0:1], turned_st[mine, 1:2]
        own = own_e[v]
        top = jnp.maximum(peak, own)
        carried, fresh = jnp.exp2(peak - top), jnp.exp2(own - top)
        u, i = v // kv, lax.rem(v, kv)
        value = own_w[u, :, pl.ds(pl.multiple_of(i * HD, HD), HD)]
        bottom = total * carried + fresh
        for g in range(GROUP):
            span = slice(g * beams, (g + 1) * beams)
            done = (numer[span] * carried[span] + fresh[span] * value) / bottom[span]
            head = pl.ds(pl.multiple_of((i * GROUP + g) * HD, HD), HD)
            out_ref[u, :, head] = done.astype(jnp.bfloat16)

    for c in taken + tables:
        c.start()
    start_fetch(0)
    barrier = pltpu.get_barrier_semaphore()
    for to in peers:
        pl.semaphore_signal(barrier, inc=1, device_id=to, device_id_type=MESH)
    pl.semaphore_wait(barrier, len(peers))

    def send_queries(v, _):
        start(v, *[("z", s) for s in in_z])
        return 0

    for c in taken:
        c.wait()
    own_copy().start()
    lax.fori_loop(0, turned_at, send_queries, 0)
    own_copy().wait()

    def send_plane(v, _):
        start(v, *[("px", b) for b in in_x], *[("py", a) for a in in_y])
        return 0

    lax.fori_loop(turned_at, chunks, send_plane, 0)
    for c in tables:
        c.wait()
    lax.fori_loop(0, users, own_terms, 0)

    def attend(v):
        @pl.when(v + 1 < chunks)
        def _():
            start_fetch(v + 1)

        gathered(v)
        for c in fetch(v):
            c.wait()
        heads(v, range(cols))
        start(v, ("f",), ("fs",))

    run = dict(
        columns=columns, relay=relay, diagonal=diagonal, attend=attend, paired=paired, crossed=crossed,
        reduced=reduced, finished=finished, delivered=delivered,
    )

    begin, end = turns(chunks)

    def each(step):
        def one(v, _):
            step(v)
            return 0

        lax.fori_loop(turned_at, chunks, one, 0)

    def turn(u, _):
        pl.when(u == begin + PLANE_CROSS)(lambda: each(plane_cross))
        pl.when(u == begin + PLANE_COLUMNS)(lambda: each(plane_columns))
        for name, base, early, late in STEPS:
            def one(v, _, name=name):
                run[name](v)
                return 0

            ends = [upto(chunks, base, early, late, x, jnp) for x in (u - 1, u)]
            lax.fori_loop(*ends, one, 0)
        return 0

    lax.fori_loop(begin, end, turn, 0)

    def close(v, _):
        def sent(names):
            for name in names:
                make(v, name).wait_send()

        sent(plan.same)
        either(v, lambda: sent(plan.usual), lambda: sent(plan.plane))
        return 0

    lax.fori_loop(0, chunks, close, 0)


def body(queries, key_cache, value_cache, key_table, value_table, lengths, token_ids):
    rows, cols = lax.axis_size("row"), lax.axis_size("col")
    plan = Plan(rows, cols)
    users, beams, _ = queries.shape
    positions = key_cache.shape[1]
    vocab = key_table.shape[0]
    kv = KH // cols
    chunks = users * kv
    lines = GROUP * beams
    lanes = CORES * lines
    outer, inner, planes, half = plan.outer, plan.inner, plan.planes, plan.half
    deep = HD // 2
    f32, bf16 = jnp.float32, jnp.bfloat16
    vmem = pl.BlockSpec(memory_space=pltpu.VMEM)
    hbm = pl.BlockSpec(memory_space=pl.ANY)
    block, stat = (deep, lanes), (2, lanes)

    def numer(*lead):
        return pltpu.VMEM((chunks, *lead, *block), bf16)

    def stats(*lead):
        return pltpu.VMEM((chunks, *lead, *stat), f32)

    x, y = max(inner - 1, 1), max(outer - 1, 1)
    copies = len(plan.same + plan.usual)
    scores = chunks * cols * planes * lanes * positions
    return pl.pallas_call(
        lambda *refs: step_kernel(plan, *refs),
        out_shape=jax.ShapeDtypeStruct(queries.shape, bf16),
        in_specs=[pl.BlockSpec(memory_space=pltpu.SMEM), vmem, hbm, hbm, hbm, hbm, hbm],
        out_specs=vmem,
        scratch_shapes=[
            pltpu.VMEM((chunks, GROUP, beams, HD), bf16),
            pltpu.VMEM((vocab, kv * HD), bf16),
            pltpu.VMEM((vocab, kv * HD), bf16),
            pltpu.VMEM((chunks, lines, 1), f32),
            pltpu.VMEM((users, beams, kv * HD), f32),
            pltpu.VMEM((lanes, HD), f32),
            pltpu.VMEM((lanes, 8), f32),
            pltpu.VMEM((chunks, 8, lanes), f32),
            pltpu.VMEM((chunks, planes, CORES, cols, GROUP, beams, HD), bf16),
            numer(2, planes, cols),
            numer(planes, cols),
            stats(planes, cols),
            stats(planes, cols),
            stats(planes, cols),
            numer(y, x, half),
            stats(y, x, half),
            numer(y, x, cols - half),
            stats(y, x, cols - half),
            numer(x, cols),
            stats(x, cols),
            numer(y, cols),
            stats(y, cols),
            numer(cols - 1),
            stats(cols - 1),
            pltpu.VMEM((chunks, 2, *block), f32),
            pltpu.VMEM((2, cols, positions, HD), bf16),
            pltpu.VMEM((2, cols, positions, HD), bf16),
            pltpu.SemaphoreType.DMA((chunks, copies)),
            pltpu.SemaphoreType.DMA((chunks, copies)),
            pltpu.SemaphoreType.DMA((1 + 4 * cols + chunks * GROUP + 2,)),
        ],
        compiler_params=pltpu.CompilerParams(
            collective_id=0, has_side_effects=True, vmem_limit_bytes=60 * 1024 * 1024
        ),
        cost_estimate=pl.CostEstimate(
            flops=4 * scores * HD, bytes_accessed=4 * key_cache.size, transcendentals=scores
        ),
        name="step",
    )(lengths, token_ids, queries, key_cache, value_cache, key_table, value_table)


def solution(mesh):
    return jax.shard_map(
        body,
        mesh=mesh,
        in_specs=(
            P(None, "row", "col"),
            P(None, ("row", "col"), None),
            P(None, ("row", "col"), None),
            P(),
            P(),
            P(),
            P(None, "row"),
        ),
        out_specs=P(None, "row", "col"),
        check_vma=False,
    )
```
